32 devices in a mesh: row: 8 (over y, x, core), col: 4 (over z).
Axes of the slice: x: 2, y: 2, z: 4, core: 2. Of those that a mesh axis runs over, the one named last changes fastest.
Arguments:
- integrals: bfloat16 [320, 32, 4096], P('row', None, 'col'), may hold values from -6 to 6
- coeffs: bfloat16 [10240, 4096], P('row', 'col'), may hold values from -0.078125 to 0.078125
- mask: int32 [320, 4], replicated, may hold values from 0 to 1, as said below
- offsets: int32 [321], replicated, may hold values from 0 to 7680, as said below
- atom_of_slot: int32 [320], replicated, may hold values from 0 to 319, as said below
Outputs:
- half_transformed: bfloat16 [4096, 4096], P('row', 'col')
The draws below stay inside these ranges and needn't reach their ends.
Inputs may be any that keep to these rules, and one draw needn't show every extreme that they name: `mask`: 1 marks a significant pair of an atom and a block of 64 window functions. offsets[0] = 0 and offsets[a + 1] - offsets[a] is atom a's number of basis functions, 16 to 32; atoms 2k and 2k + 1 together have 3 * 16; rows of an atom's padded block past its number are padding. `atom_of_slot`: a permutation of the atoms; slot k is held by atom owner k // 40 along row, and atom a's AO-row owner is a // 40; one atom owner holds at least one and at most 5 atoms of any one AO-row owner, and exactly 5 for some pairs.
All inputs are finite; a program needn't handle non-finite values.
Results may differ from the reference program's by a relative error of at most 0.015.
Values may be sent and summed in bfloat16 or wider, within the bound.
No kernel may reach another device: no remote copies, remote signals or barrier semaphores. Data moves between devices by JAX's collectives and lax.ppermute only.
A program may use at most 256 MiB of HBM per device.

```python
import jax
import jax.numpy as jnp
from jax import lax

AW = 32
ATOMS_DEV = 40
NOCC = 4096
NAUX = 16
NU_DEV = 64
NATOM = 320
NBAS = 10240
NU = 256
NVB = 4
CAP = 5
N_ROW = 8


def draw_mask(key, part):
    first_key = jax.random.fold_in(key, 11)
    second_key = jax.random.fold_in(key, 12)
    percent = jax.random.randint(first_key, (N_ROW,), 10, 96)
    rolled = jax.random.randint(second_key, (NATOM, NVB), 0, 100)
    owner = jnp.arange(NATOM, dtype=jnp.int32) // ATOMS_DEV
    return (rolled < percent[owner][:, None]).astype(jnp.int32)


def draw_offsets(key, part):
    firsts = jax.random.randint(jax.random.fold_in(key, 21), (NATOM // 2,), AW // 2, AW + 1)
    seconds = 3 * AW // 2 - firsts
    counts = jnp.stack([firsts, seconds], axis=1).reshape(-1).astype(jnp.int32)
    return jnp.concatenate([jnp.zeros((1,), jnp.int32), jnp.cumsum(counts).astype(jnp.int32)])


def draw_atom_of_slot(key, part):
    first_key = jax.random.fold_in(key, 31)
    second_key = jax.random.fold_in(key, 32)
    third_key = jax.random.fold_in(key, 33)
    fourth_key = jax.random.fold_in(key, 34)
    every_shift = jax.random.permutation(first_key, jnp.arange(N_ROW, dtype=jnp.int32))
    repeated = jnp.tile(jnp.arange(N_ROW, dtype=jnp.int32), CAP - 1)
    extra = jax.random.permutation(third_key, repeated)[:ATOMS_DEV - N_ROW]
    shifts = jax.random.permutation(fourth_key, jnp.concatenate([every_shift, extra]).astype(jnp.int32))
    locals_table = jax.vmap(lambda owner: jax.random.permutation(jax.random.fold_in(second_key, owner), ATOMS_DEV))(jnp.arange(N_ROW, dtype=jnp.int32))
    source = jnp.arange(N_ROW, dtype=jnp.int32)[:, None]
    layer = jnp.arange(ATOMS_DEV, dtype=jnp.int32)[None, :]
    target = (source - shifts[None, :]) % N_ROW
    chosen = locals_table[target, jnp.broadcast_to(layer, target.shape)].astype(jnp.int32)
    return (target * ATOMS_DEV + chosen).reshape(-1).astype(jnp.int32)


def strengthened(drawn, stream_key, source, target, parts, factor):
    def block_of(axis_at):
        return (jnp.arange(drawn.shape[axis_at]) // (drawn.shape[axis_at] // parts)).reshape((-1,) + (1,) * (drawn.ndim - 1 - axis_at))

    one_side = jax.random.permutation(stream_key, parts)[block_of(target)]
    second = (block_of(target) + parts // 2) % parts
    return jnp.where((block_of(source) == one_side) | (block_of(source) == second), factor * drawn, drawn)


def block_levels(rng, dims, split, smallest, largest):
    level = 1.0
    for position, shards_of in split:
        steps = jax.random.uniform(jax.random.fold_in(jax.random.fold_in(rng, 6), position), (shards_of,), jnp.float32, smallest / len(split), largest / len(split))
        level = level * jnp.repeat(jnp.exp(steps), dims[position] // shards_of).reshape((-1,) + (1,) * (len(dims) - 1 - position))
    return level


def normal_values(own_key, extent, spread, bound, shards=(), kind=jnp.bfloat16):
    result = spread * jax.random.normal(own_key, extent, jnp.float32)
    if shards:
        result = result * block_levels(own_key, extent, shards, -0.22, 0.18)
    return jnp.clip(result, -bound, bound).astype(kind)


def gaussian_with(rng, dims, scale, reach, cuts, heavy, held_as=jnp.bfloat16):
    drawn = scale * jax.random.normal(rng, dims, jnp.float32)
    if cuts:
        drawn = drawn * block_levels(rng, dims, cuts, -0.22, 0.18)
    return jnp.clip(strengthened(drawn, jax.random.fold_in(rng, 3), *heavy), -reach, reach).astype(held_as)


def setup_inputs(seed: int = 0) -> dict:
    key_list = jax.random.split(jax.random.key(seed), 6)
    return {
        "integrals": normal_values(key_list[0], (NATOM, AW, NU * NAUX), 1.0, 6.0, ((0, 8), (2, 4))),
        "coeffs": gaussian_with(key_list[1], (NBAS, NOCC), NBAS ** -0.5, 0.078125, ((0, 8), (1, 4)), (0, 1, 8, 2.0)),
        "mask": draw_mask(jax.random.fold_in(key_list[5], 71), 0),
        "offsets": draw_offsets(jax.random.fold_in(key_list[5], 71), 0),
        "atom_of_slot": draw_atom_of_slot(jax.random.fold_in(key_list[5], 71), 0),
    }


def reference(integrals, coeffs, mask, offsets, atom_of_slot):
    natoms = integrals.shape[0]
    inverse = jnp.zeros((natoms,), jnp.int32).at[atom_of_slot].set(jnp.arange(natoms, dtype=jnp.int32))
    ordered = integrals[inverse]
    lengths = offsets[1:] - offsets[:-1]
    row_live = (jnp.arange(AW, dtype=jnp.int32)[None, :] < lengths[:, None]).astype(jnp.bfloat16)
    column_live = jnp.repeat(mask, NU_DEV * NAUX, axis=1).astype(jnp.bfloat16)
    kept = ordered * row_live[:, :, None] * column_live[:, None, :]
    width = kept.shape[2]
    kept_groups = kept.reshape(N_ROW, ATOMS_DEV * AW, width)
    coeff_groups = coeffs.reshape(N_ROW, ATOMS_DEV * AW, coeffs.shape[1])

    def add_owner(total, pieces):
        coeff_piece, kept_piece = pieces
        part = lax.dot_general(coeff_piece, kept_piece, (((0,), (0,)), ((), ())), preferred_element_type=jnp.float32)
        part = lax.optimization_barrier(part.astype(jnp.bfloat16))
        return total + part.astype(jnp.float32), None

    start = jnp.zeros((coeffs.shape[1], width), jnp.float32)
    half, unused = lax.scan(add_owner, start, (coeff_groups, kept_groups))
    return half.astype(jnp.bfloat16)
```

```python
import functools
import jax
import jax.numpy as jnp
from jax import lax
from jax.experimental import pallas as pl
from jax.experimental.pallas import tpu as pltpu
from jax.sharding import PartitionSpec as P


LANES = 256


def selector(first, alive, atom_w, group):
    pair_w = 3 * atom_w // 2
    rows, cols = group // 2 * pair_w, group * atom_w
    row = lax.broadcasted_iota(jnp.int32, (rows, cols), 0)
    col = lax.broadcasted_iota(jnp.int32, (rows, cols), 1)
    wanted = jnp.full((rows, cols), -1, jnp.int32)
    for pair in range(group // 2):
        inside = row - pair * pair_w
        in_first = inside < first[pair]
        source = jnp.where(in_first, inside, inside + atom_w - first[pair]) + 2 * pair * atom_w
        if alive is not None:
            live = jnp.where(in_first, alive[2 * pair], alive[2 * pair + 1]) > 0
            source = jnp.where(live, source, -1)
        wanted = jnp.where((inside >= 0) & (inside < pair_w), source, wanted)
    return (wanted == col).astype(jnp.bfloat16)


def pack_coeffs_kernel(atom_w, group, widths, lengths, core, coeffs, *pieces):
    step = pl.program_id(0)
    first = [lengths[step * group + 2 * pair] for pair in range(group // 2)]
    chooser = selector(first, None, atom_w, group)
    half = sum(widths)
    for side in range(2):
        start = half * jnp.where(core[0] == side, 0, 1)
        for which, width in enumerate(widths):
            offset = pl.multiple_of(start + sum(widths[:which]), 128)
            block = coeffs[:, pl.ds(offset, width)]
            pieces[side * len(widths) + which][...] = jnp.dot(
                chooser, block, preferred_element_type=jnp.float32
            ).astype(jnp.bfloat16)


def pack_coeffs(coeffs, lengths, core, per_dev, atom_w, group, widths):
    rows_in, rows_out = group * atom_w, group // 2 * (3 * atom_w // 2)
    steps = per_dev // group
    smem = pl.BlockSpec(memory_space=pltpu.SMEM)
    return pl.pallas_call(
        functools.partial(pack_coeffs_kernel, atom_w, group, widths),
        grid=(steps,),
        in_specs=[smem, smem, pl.BlockSpec((rows_in, coeffs.shape[1]), lambda i: (i, 0))],
        out_specs=[pl.BlockSpec((rows_out, w), lambda i: (i, 0)) for w in widths * 2],
        out_shape=[jax.ShapeDtypeStruct((steps * rows_out, w), jnp.bfloat16) for w in widths * 2],
        name="pack_coeffs",
    )(lengths, core, coeffs)


def sort_blocks_kernel(slots, table, blocks, *outs):
    for which, out in enumerate(outs):
        for rank in range(2 * slots):
            out[rank] = blocks[table[which * 2 * slots + rank]]


def sort_blocks(blocks, table, n_chip, slots):
    shape = (2 * slots,) + blocks.shape[1:]
    vmem = pl.BlockSpec(memory_space=pltpu.VMEM)
    return pl.pallas_call(
        functools.partial(sort_blocks_kernel, slots),
        in_specs=[pl.BlockSpec(memory_space=pltpu.SMEM), vmem],
        out_specs=[vmem] * n_chip,
        out_shape=[jax.ShapeDtypeStruct(shape, blocks.dtype)] * n_chip,
        name="sort_blocks",
    )(table, blocks)


def pack_kept_kernel(n_in, slots, atom_w, group, where_of, lengths, alive, *refs):
    arrived, out, stack, window = refs[:n_in], refs[n_in], refs[n_in + 1], refs[n_in + 2]
    for which in range(n_in - 1):
        stack[which * slots : (which + 1) * slots] = arrived[which][:slots]
    stack[(n_in - 1) * slots :] = arrived[n_in - 1][...]
    rows_out = group // 2 * (3 * atom_w // 2)
    for step in range(out.shape[0] // rows_out):
        base = step * group
        for atom in range(group):
            window[atom * atom_w : (atom + 1) * atom_w, :] = stack[where_of[base + atom]]
        first = [lengths[base + 2 * pair] for pair in range(group // 2)]
        chooser = selector(first, [alive[base + i] for i in range(group)], atom_w, group)
        out[step * rows_out : (step + 1) * rows_out, :] = jnp.dot(
            chooser, window[...], preferred_element_type=jnp.float32
        ).astype(jnp.bfloat16)


def pack_kept(arrived, where_of, lengths, alive, atom_w, group):
    slots, width = arrived[0].shape[0] // 2, arrived[0].shape[2]
    per_dev = where_of.shape[0]
    smem, vmem = pl.BlockSpec(memory_space=pltpu.SMEM), pl.BlockSpec(memory_space=pltpu.VMEM)
    return pl.pallas_call(
        functools.partial(pack_kept_kernel, len(arrived), slots, atom_w, group),
        in_specs=[smem] * 3 + [vmem] * len(arrived),
        out_specs=vmem,
        out_shape=jax.ShapeDtypeStruct((per_dev // 2 * (3 * atom_w // 2), width), jnp.bfloat16),
        scratch_shapes=[
            pltpu.VMEM((per_dev, atom_w, width), jnp.bfloat16),
            pltpu.VMEM((group * atom_w, width), jnp.bfloat16),
        ],
        name="pack_kept",
    )(where_of, lengths, alive, *arrived)


def block_tables(atom_of_slot, own_row, n_row, per_dev, slots):
    counter = jnp.arange(per_dev, dtype=jnp.int32)
    holders = atom_of_slot.reshape(n_row, per_dev)
    owner = holders // per_dev
    earlier = (owner[:, None, :] == owner[:, :, None]) & (counter[None, :] < counter[:, None])[None]
    rank = jnp.sum(earlier.astype(jnp.int32), axis=2)
    mine_owner = lax.dynamic_slice_in_dim(owner, own_row, 1)[0]
    mine_rank = lax.dynamic_slice_in_dim(rank, own_row, 1)[0]
    place = (mine_owner ^ own_row) * slots + mine_rank
    table = jnp.sum(jnp.where(place[None, :] == counter[:, None], counter[None, :], 0), axis=1)
    apart = jnp.arange(n_row, dtype=jnp.int32)[:, None] ^ own_row
    arrival = ((apart % 2) * (n_row // 2) + apart // 2) * slots + rank
    local = holders.reshape(-1) - own_row * per_dev
    where_of = jnp.sum(
        jnp.where(local[None, :] == counter[:, None], arrival.reshape(-1)[None, :], 0), axis=1
    )
    return table, where_of


def products_kernel(n_stream, choice, kept, kept_pair, *refs):
    streams, outs = refs[:n_stream], refs[n_stream : n_stream + len(refs) - n_stream - 2]
    buffer, sems = refs[-2], refs[-1]
    width = outs[0].shape[0]

    def fetch(step):
        for which in range(n_stream):

            @pl.when(choice[step] == which)
            def _():
                pltpu.make_async_copy(
                    streams[which], buffer.at[step % 2], sems.at[step % 2]
                ).start()

    fetch(0)
    for step, out in enumerate(outs):
        if step + 1 < len(outs):
            fetch(step + 1)
        pltpu.make_async_copy(streams[0], buffer.at[step % 2], sems.at[step % 2]).wait()
        dims = (((0,), (0,)), ((), ()))
        total = lax.dot_general(
            buffer[step % 2, :, :width], kept[...], dims, preferred_element_type=jnp.float32
        )
        total += lax.dot_general(
            buffer[step % 2, :, width:], kept_pair[...], dims, preferred_element_type=jnp.float32
        )
        out[...] = total.astype(out.dtype)


def products(choice, kept, kept_pair, streams, n_out):
    rows, both = streams[0].shape
    width, columns = both // 2, kept.shape[1]
    vmem = pl.BlockSpec(memory_space=pltpu.VMEM)
    flops = n_out * 2 * both * rows * columns
    return pl.pallas_call(
        functools.partial(products_kernel, len(streams)),
        in_specs=[pl.BlockSpec(memory_space=pltpu.SMEM), vmem, vmem]
        + [pl.BlockSpec(memory_space=pl.ANY)] * len(streams),
        out_specs=[vmem] * n_out,
        out_shape=[jax.ShapeDtypeStruct((width, columns), jnp.bfloat16)] * n_out,
        scratch_shapes=[
            pltpu.VMEM((2, rows, both), jnp.bfloat16),
            pltpu.SemaphoreType.DMA((2,)),
        ],
        cost_estimate=pl.CostEstimate(flops=flops, bytes_accessed=flops // 512, transcendentals=0),
        name="products",
    )(choice, kept, kept_pair, *streams)


def line_body(integrals, coeffs, mask, offsets, atom_of_slot):
    n_row, n_col = lax.axis_size("row"), lax.axis_size("col")
    own_row, own_col = lax.axis_index("row"), lax.axis_index("col")
    per_dev, atom_w, _ = integrals.shape
    slots = per_dev // n_row
    group = LANES // atom_w
    core, chip = own_row % 2, own_row // 2
    n_chip = n_row // 2
    half = coeffs.shape[1] // 2
    widths = (half // 2, half // 4, half // 4)
    n_piece = len(widths)

    bounds = lax.dynamic_slice_in_dim(offsets, own_row * per_dev, per_dev + 1)
    lengths = bounds[1:] - bounds[:-1]
    core_arg = core.astype(jnp.int32).reshape(1)

    swap = [(r, r ^ 1) for r in range(n_row)]
    pieces = pack_coeffs(coeffs, lengths, core_arg, per_dev, atom_w, group, (half,))
    paired = lax.ppermute(pieces[1], "row", swap)
    units = []
    for which in range(n_piece):
        cut = slice(sum(widths[:which]), sum(widths[: which + 1]))
        units.append(jnp.concatenate([pieces[0][:, cut], paired[:, cut]], axis=1))

    right = [(c, c + 1) for c in range(n_col - 1)]
    left = [(c + 1, c) for c in range(n_col - 1)]
    from_left = [lax.ppermute(unit, "col", right) for unit in units]
    from_right = [lax.ppermute(unit, "col", left) for unit in units]

    table, where_of = block_tables(atom_of_slot, own_row, n_row, per_dev, slots)
    alive = lax.dynamic_slice(mask, (own_row * per_dev, own_col), (per_dev, 1))[:, 0]
    outgoing = sort_blocks(integrals, table, n_chip, slots)
    arrived = [outgoing[0]] + [
        lax.ppermute(outgoing[d], "row", [(r, r ^ (2 * d)) for r in range(n_row)])
        for d in range(1, n_chip)
    ]
    theirs = jnp.concatenate([block[slots:] for block in arrived], axis=0)
    arrived.append(lax.ppermute(theirs, "row", swap))
    kept = pack_kept(arrived, where_of, lengths, alive, atom_w, group)
    kept_pair = lax.ppermute(kept, "row", swap)

    far_left = [lax.ppermute(unit, "col", right[1:]) for unit in from_left]
    far_right = [lax.ppermute(unit, "col", left[:-1]) for unit in from_right]
    on_left = own_col < n_col // 2
    third = [
        lax.ppermute(jnp.where(on_left, r, l), "col", [(1, 0), (n_col - 2, n_col - 1)])
        for l, r in zip(far_left, far_right)
    ]

    goals = chip ^ jnp.arange(n_chip, dtype=jnp.int32)
    gap = goals - own_col
    choice = jnp.full((n_chip,), 5, jnp.int32)
    for value, which in ((0, 0), (-1, 1), (1, 2), (-2, 3), (2, 4)):
        choice = jnp.where(gap == value, which, choice)
    rows = []
    for which in range(n_piece):
        streams = [
            group_of[which]
            for group_of in (units, from_left, from_right, far_left, far_right, third)
        ]
        parts = products(choice, kept, kept_pair, streams, n_chip)
        total = parts[0].astype(jnp.float32)
        for d in range(1, n_chip):
            perm = [(r, r ^ (2 * d)) for r in range(n_row)]
            total = total + lax.ppermute(parts[d], "row", perm).astype(jnp.float32)
        rows.append(total.astype(jnp.bfloat16))
    return jnp.concatenate(rows, axis=0)


def body(integrals, coeffs, mask, offsets, atom_of_slot):
    n_row = lax.axis_size("row")
    own_row = lax.axis_index("row")
    own_col = lax.axis_index("col")
    per_dev, atom_w, row_width = integrals.shape
    slots_cap = max(2, -(-per_dev // n_row))
    counter = jnp.arange(per_dev, dtype=jnp.int32)
    slot_count = n_row * slots_cap
    mine_slots = lax.dynamic_slice_in_dim(atom_of_slot, own_row * per_dev, per_dev)
    target = mine_slots // per_dev
    before = (target[None, :] == target[:, None]) & (counter[None, :] < counter[:, None])
    arrival_rank = jnp.sum(before.astype(jnp.int32), axis=1)
    position = target * slots_cap + arrival_rank
    placing = (jnp.arange(slot_count, dtype=jnp.int32)[:, None] == position[None, :]).astype(
        jnp.bfloat16
    )
    outgoing = jnp.dot(
        placing, integrals.reshape(per_dev, atom_w * row_width), preferred_element_type=jnp.bfloat16
    )
    outgoing = outgoing.reshape(n_row, slots_cap, atom_w * row_width)
    incoming = lax.all_to_all(outgoing, "row", split_axis=0, concat_axis=0, tiled=True)
    holders = atom_of_slot.reshape(n_row, per_dev)
    is_mine = holders // per_dev == own_row
    arrival = jnp.cumsum(is_mine.astype(jnp.int32), axis=1) - 1
    slot_of = jnp.arange(n_row, dtype=jnp.int32)[:, None] * slots_cap + arrival
    local_atom = holders - own_row * per_dev
    pick_atom = (
        (local_atom.reshape(-1)[:, None] == counter[None, :]) & is_mine.reshape(-1)[:, None]
    ).astype(jnp.float32)
    pick_slot = (
        slot_of.reshape(-1)[:, None] == jnp.arange(slot_count, dtype=jnp.int32)[None, :]
    ).astype(jnp.float32)
    gather_matrix = jnp.dot(pick_atom.T, pick_slot).astype(jnp.bfloat16)
    ordered = jnp.dot(
        gather_matrix,
        incoming.reshape(slot_count, atom_w * row_width),
        preferred_element_type=jnp.bfloat16,
    )
    ordered = ordered.reshape(per_dev, atom_w, row_width)
    bounds = lax.dynamic_slice_in_dim(offsets, own_row * per_dev, per_dev + 1)
    lengths = bounds[1:] - bounds[:-1]
    significant = lax.dynamic_slice(mask, (own_row * per_dev, own_col), (per_dev, 1))[:, 0] > 0
    keep_rows = (jnp.arange(atom_w, dtype=jnp.int32)[None, :] < lengths[:, None]) & significant[
        :, None
    ]
    blocks = ordered * keep_rows[:, :, None].astype(jnp.bfloat16)
    kept_rows = blocks.reshape(per_dev * atom_w, row_width)
    coeff_piece = lax.all_gather(coeffs, "col", axis=1, tiled=True)

    def product():
        return lax.dot_general(
            coeff_piece, kept_rows, (((0,), (0,)), ((), ())), preferred_element_type=jnp.float32
        )

    bucket_term = product()
    partial_sums = bucket_term.astype(jnp.bfloat16)
    result = lax.psum_scatter(partial_sums, "row", scatter_dimension=0, tiled=True).astype(
        jnp.float32
    )
    return result.astype(jnp.bfloat16)


def solution(mesh):
    in_specs = (P("row", None, "col"), P("row", "col"), P(), P(), P())
    out_specs = P("row", "col")
    n_row, n_col = mesh.shape["row"], mesh.shape["col"]

    def step(integrals, coeffs, mask, offsets, atom_of_slot):
        even = integrals.shape[0] % (n_row * n_row) == 0
        chosen = line_body if even and n_col == 4 and n_row == 2 * n_col else body
        mapped = jax.shard_map(
            chosen, mesh=mesh, in_specs=in_specs, out_specs=out_specs, check_vma=False
        )
        return mapped(integrals, coeffs, mask, offsets, atom_of_slot)

    return step
```

```python
import functools
import jax
import jax.numpy as jnp
from jax import lax
from jax.experimental import pallas as pl
from jax.experimental.pallas import tpu as pltpu
from jax.sharding import PartitionSpec as P


LANES = 256


def selector(first, alive, atom_w, group):
    pair_w = 3 * atom_w // 2
    rows, cols = group // 2 * pair_w, group * atom_w
    row = lax.broadcasted_iota(jnp.int32, (rows, cols), 0)
    col = lax.broadcasted_iota(jnp.int32, (rows, cols), 1)
    wanted = jnp.full((rows, cols), -1, jnp.int32)
    for pair in range(group // 2):
        inside = row - pair * pair_w
        in_first = inside < first[pair]
        source = jnp.where(in_first, inside, inside + atom_w - first[pair]) + 2 * pair * atom_w
        if alive is not None:
            live = jnp.where(in_first, alive[2 * pair], alive[2 * pair + 1]) > 0
            source = jnp.where(live, source, -1)
        wanted = jnp.where((inside >= 0) & (inside < pair_w), source, wanted)
    return (wanted == col).astype(jnp.bfloat16)


def pack_coeffs_kernel(atom_w, group, widths, lengths, core, coeffs, *pieces):
    step = pl.program_id(0)
    first = [lengths[step * group + 2 * pair] for pair in range(group // 2)]
    chooser = selector(first, None, atom_w, group)
    half = sum(widths)
    for side in range(2):
        start = half * jnp.where(core[0] == side, 0, 1)
        for which, width in enumerate(widths):
            offset = pl.multiple_of(start + sum(widths[:which]), 128)
            block = coeffs[:, pl.ds(offset, width)]
            pieces[side * len(widths) + which][...] = jnp.dot(
                chooser, block, preferred_element_type=jnp.float32
            ).astype(jnp.bfloat16)


def pack_coeffs(coeffs, lengths, core, per_dev, atom_w, group, widths):
    rows_in, rows_out = group * atom_w, group // 2 * (3 * atom_w // 2)
    steps = per_dev // group
    smem = pl.BlockSpec(memory_space=pltpu.SMEM)
    return pl.pallas_call(
        functools.partial(pack_coeffs_kernel, atom_w, group, widths),
        grid=(steps,),
        in_specs=[smem, smem, pl.BlockSpec((rows_in, coeffs.shape[1]), lambda i: (i, 0))],
        out_specs=[pl.BlockSpec((rows_out, w), lambda i: (i, 0)) for w in widths * 2],
        out_shape=[jax.ShapeDtypeStruct((steps * rows_out, w), jnp.bfloat16) for w in widths * 2],
        name="pack_coeffs",
    )(lengths, core, coeffs)


def sort_blocks_kernel(slots, table, blocks, *outs):
    for which, out in enumerate(outs):
        for rank in range(2 * slots):
            out[rank] = blocks[table[which * 2 * slots + rank]]


def sort_blocks(blocks, table, n_chip, slots):
    shape = (2 * slots,) + blocks.shape[1:]
    vmem = pl.BlockSpec(memory_space=pltpu.VMEM)
    return pl.pallas_call(
        functools.partial(sort_blocks_kernel, slots),
        in_specs=[pl.BlockSpec(memory_space=pltpu.SMEM), vmem],
        out_specs=[vmem] * n_chip,
        out_shape=[jax.ShapeDtypeStruct(shape, blocks.dtype)] * n_chip,
        name="sort_blocks",
    )(table, blocks)


def pack_kept_kernel(n_in, slots, atom_w, group, where_of, lengths, alive, *refs):
    arrived, out, stack, window = refs[:n_in], refs[n_in], refs[n_in + 1], refs[n_in + 2]
    for which in range(n_in - 1):
        stack[which * slots : (which + 1) * slots] = arrived[which][:slots]
    stack[(n_in - 1) * slots :] = arrived[n_in - 1][...]
    rows_out = group // 2 * (3 * atom_w // 2)
    for step in range(out.shape[0] // rows_out):
        base = step * group
        for atom in range(group):
            window[atom * atom_w : (atom + 1) * atom_w, :] = stack[where_of[base + atom]]
        first = [lengths[base + 2 * pair] for pair in range(group // 2)]
        chooser = selector(first, [alive[base + i] for i in range(group)], atom_w, group)
        out[step * rows_out : (step + 1) * rows_out, :] = jnp.dot(
            chooser, window[...], preferred_element_type=jnp.float32
        ).astype(jnp.bfloat16)


def pack_kept(arrived, where_of, lengths, alive, atom_w, group):
    slots, width = arrived[0].shape[0] // 2, arrived[0].shape[2]
    per_dev = where_of.shape[0]
    smem, vmem = pl.BlockSpec(memory_space=pltpu.SMEM), pl.BlockSpec(memory_space=pltpu.VMEM)
    return pl.pallas_call(
        functools.partial(pack_kept_kernel, len(arrived), slots, atom_w, group),
        in_specs=[smem] * 3 + [vmem] * len(arrived),
        out_specs=vmem,
        out_shape=jax.ShapeDtypeStruct((per_dev // 2 * (3 * atom_w // 2), width), jnp.bfloat16),
        scratch_shapes=[
            pltpu.VMEM((per_dev, atom_w, width), jnp.bfloat16),
            pltpu.VMEM((group * atom_w, width), jnp.bfloat16),
        ],
        name="pack_kept",
    )(where_of, lengths, alive, *arrived)


def block_tables(atom_of_slot, own_row, n_row, per_dev, slots):
    counter = jnp.arange(per_dev, dtype=jnp.int32)
    holders = atom_of_slot.reshape(n_row, per_dev)
    owner = holders // per_dev
    earlier = (owner[:, None, :] == owner[:, :, None]) & (counter[None, :] < counter[:, None])[None]
    rank = jnp.sum(earlier.astype(jnp.int32), axis=2)
    mine_owner = lax.dynamic_slice_in_dim(owner, own_row, 1)[0]
    mine_rank = lax.dynamic_slice_in_dim(rank, own_row, 1)[0]
    place = (mine_owner ^ own_row) * slots + mine_rank
    table = jnp.sum(jnp.where(place[None, :] == counter[:, None], counter[None, :], 0), axis=1)
    apart = jnp.arange(n_row, dtype=jnp.int32)[:, None] ^ own_row
    arrival = ((apart % 2) * (n_row // 2) + apart // 2) * slots + rank
    local = holders.reshape(-1) - own_row * per_dev
    where_of = jnp.sum(
        jnp.where(local[None, :] == counter[:, None], arrival.reshape(-1)[None, :], 0), axis=1
    )
    return table, where_of


def products_kernel(candidates, choice, kept, kept_pair, *refs):
    n_ref = 1 + max(ref for ref, _, _ in candidates)
    streams, outs = refs[:n_ref], refs[n_ref:-2]
    buffer, sem = refs[-2], refs[-1]
    width = outs[0].shape[0]
    half = width * len(outs)

    def pull(ref, offset, place):
        return pltpu.make_async_copy(
            streams[ref].at[:, pl.ds(offset, width)], buffer.at[:, pl.ds(place, width)], sem
        )

    for step in range(len(outs)):
        for which, (ref, own, pair) in enumerate(candidates):

            @pl.when(choice[step] == which)
            def _():
                pull(ref, own, step * width).start()
                pull(ref, pair, half + step * width).start()

    for step in range(2 * len(outs)):
        pull(0, 0, step * width).wait()
    dims = (((0,), (0,)), ((), ()))
    total = lax.dot_general(
        buffer[:, :half], kept[...], dims, preferred_element_type=jnp.float32
    ) + lax.dot_general(
        buffer[:, half:], kept_pair[...], dims, preferred_element_type=jnp.float32
    )
    for step, out in enumerate(outs):
        out[...] = total[step * width : (step + 1) * width].astype(out.dtype)


def products(choice, kept, kept_pair, streams, candidates, n_out, width):
    rows, columns = kept.shape
    vmem = pl.BlockSpec(memory_space=pltpu.VMEM)
    flops = n_out * 4 * width * rows * columns
    return pl.pallas_call(
        functools.partial(products_kernel, candidates),
        in_specs=[pl.BlockSpec(memory_space=pltpu.SMEM), vmem, vmem]
        + [pl.BlockSpec(memory_space=pl.ANY)] * len(streams),
        out_specs=[vmem] * n_out,
        out_shape=[jax.ShapeDtypeStruct((width, columns), jnp.bfloat16)] * n_out,
        scratch_shapes=[
            pltpu.VMEM((rows, 2 * n_out * width), jnp.bfloat16),
            pltpu.SemaphoreType.DMA,
        ],
        cost_estimate=pl.CostEstimate(flops=flops, bytes_accessed=flops // 512, transcendentals=0),
        name="products",
    )(choice, kept, kept_pair, *streams)


def line_body(integrals, coeffs, mask, offsets, atom_of_slot):
    n_row, n_col = lax.axis_size("row"), lax.axis_size("col")
    own_row, own_col = lax.axis_index("row"), lax.axis_index("col")
    per_dev, atom_w, _ = integrals.shape
    slots = per_dev // n_row
    group = LANES // atom_w
    core, chip = own_row % 2, own_row // 2
    n_chip = n_row // 2
    half = coeffs.shape[1] // 2
    widths = (half // 2, half // 4, half // 4)
    n_piece = len(widths)
    last = n_col - 1

    bounds = lax.dynamic_slice_in_dim(offsets, own_row * per_dev, per_dev + 1)
    lengths = bounds[1:] - bounds[:-1]
    core_arg = core.astype(jnp.int32).reshape(1)

    swap = [(r, r ^ 1) for r in range(n_row)]
    pieces = pack_coeffs(coeffs, lengths, core_arg, per_dev, atom_w, group, (half,))
    paired = lax.ppermute(pieces[1], "row", swap)
    units = []
    for which in range(n_piece):
        cut = slice(sum(widths[:which]), sum(widths[: which + 1]))
        units.append(jnp.concatenate([pieces[0][:, cut], paired[:, cut]], axis=1))

    right = [(c, c + 1) for c in range(n_col - 1)]
    left = [(c + 1, c) for c in range(n_col - 1)]
    from_left = [lax.ppermute(unit, "col", right) for unit in units]
    from_right = [lax.ppermute(unit, "col", left) for unit in units]

    table, where_of = block_tables(atom_of_slot, own_row, n_row, per_dev, slots)
    alive = lax.dynamic_slice(mask, (own_row * per_dev, own_col), (per_dev, 1))[:, 0]
    outgoing = sort_blocks(integrals, table, n_chip, slots)
    arrived = [outgoing[0]] + [
        lax.ppermute(outgoing[d], "row", [(r, r ^ (2 * d)) for r in range(n_row)])
        for d in range(1, n_chip)
    ]
    theirs = jnp.concatenate([block[slots:] for block in arrived], axis=0)
    arrived.append(lax.ppermute(theirs, "row", swap))
    kept = pack_kept(arrived, where_of, lengths, alive, atom_w, group)
    kept_pair = lax.ppermute(kept, "row", swap)

    far_left = [lax.ppermute(unit, "col", right[1:]) for unit in from_left]
    far_right = [lax.ppermute(unit, "col", left[:-1]) for unit in from_right]
    on_left = own_col < n_col // 2
    helped = lax.ppermute(kept, "col", [(0, 1), (last, last - 1)])
    helped_pair = lax.ppermute(helped, "row", swap)

    goals = chip ^ jnp.arange(n_chip, dtype=jnp.int32)
    gap = goals - own_col
    choice = jnp.zeros((n_chip,), jnp.int32)
    for value, which in ((-1, 1), (1, 2), (-2, 3), (2, 4)):
        choice = jnp.where(gap == value, which, choice)
    totals = []
    for which, width in enumerate(widths):
        streams = [
            group_of[which] for group_of in (units, from_left, from_right, far_left, far_right)
        ]
        candidates = tuple((ref, 0, width) for ref in range(len(streams)))
        parts = products(choice, kept, kept_pair, streams, candidates, n_chip, width)
        total = parts[0].astype(jnp.float32)
        for d in range(1, n_chip):
            perm = [(r, r ^ (2 * d)) for r in range(n_row)]
            total = total + lax.ppermute(parts[d], "row", perm).astype(jnp.float32)
        totals.append(total)

    quarter = half // n_chip
    candidates = []
    for q in range(n_chip):
        begin, piece = q * quarter, 0
        while begin >= widths[piece]:
            begin, piece = begin - widths[piece], piece + 1
        for side in range(2):
            candidates.append((side * n_piece + piece, begin, widths[piece] + begin))
    choice = 2 * goals + on_left.astype(jnp.int32)
    parts = products(
        choice, helped, helped_pair, far_left + far_right, tuple(candidates), n_chip, quarter
    )
    total = parts[0].astype(jnp.float32)
    for d in range(1, n_chip):
        perm = [(r, r ^ (2 * d)) for r in range(n_row)]
        total = total + lax.ppermute(parts[d], "row", perm).astype(jnp.float32)
    total = total.astype(jnp.bfloat16)
    given = []
    for d in range(n_chip):
        perm = [
            (((p ^ d) * 2 + s) * n_col + source, (p * 2 + s) * n_col + goal)
            for source, goal, p in ((1, 0, last), (last - 1, last, 0))
            for s in range(2)
        ]
        given.append(lax.ppermute(total, ("row", "col"), perm))
    is_helped = ((own_col == 0) & (chip == last)) | ((own_col == last) & (chip == 0))
    rows, begin = [], 0
    for total, width in zip(totals, widths):
        gifts = [
            jnp.where(on_left, given[q ^ last], given[q])
            for q in range(begin // quarter, (begin + width) // quarter)
        ]
        rows.append(jnp.where(is_helped, jnp.concatenate(gifts), total.astype(jnp.bfloat16)))
        begin += width
    return jnp.concatenate(rows, axis=0)


def body(integrals, coeffs, mask, offsets, atom_of_slot):
    n_row = lax.axis_size("row")
    own_row = lax.axis_index("row")
    own_col = lax.axis_index("col")
    per_dev, atom_w, row_width = integrals.shape
    slots_cap = max(2, -(-per_dev // n_row))
    counter = jnp.arange(per_dev, dtype=jnp.int32)
    slot_count = n_row * slots_cap
    mine_slots = lax.dynamic_slice_in_dim(atom_of_slot, own_row * per_dev, per_dev)
    target = mine_slots // per_dev
    before = (target[None, :] == target[:, None]) & (counter[None, :] < counter[:, None])
    arrival_rank = jnp.sum(before.astype(jnp.int32), axis=1)
    position = target * slots_cap + arrival_rank
    placing = (jnp.arange(slot_count, dtype=jnp.int32)[:, None] == position[None, :]).astype(
        jnp.bfloat16
    )
    outgoing = jnp.dot(
        placing, integrals.reshape(per_dev, atom_w * row_width), preferred_element_type=jnp.bfloat16
    )
    outgoing = outgoing.reshape(n_row, slots_cap, atom_w * row_width)
    incoming = lax.all_to_all(outgoing, "row", split_axis=0, concat_axis=0, tiled=True)
    holders = atom_of_slot.reshape(n_row, per_dev)
    is_mine = holders // per_dev == own_row
    arrival = jnp.cumsum(is_mine.astype(jnp.int32), axis=1) - 1
    slot_of = jnp.arange(n_row, dtype=jnp.int32)[:, None] * slots_cap + arrival
    local_atom = holders - own_row * per_dev
    pick_atom = (
        (local_atom.reshape(-1)[:, None] == counter[None, :]) & is_mine.reshape(-1)[:, None]
    ).astype(jnp.float32)
    pick_slot = (
        slot_of.reshape(-1)[:, None] == jnp.arange(slot_count, dtype=jnp.int32)[None, :]
    ).astype(jnp.float32)
    gather_matrix = jnp.dot(pick_atom.T, pick_slot).astype(jnp.bfloat16)
    ordered = jnp.dot(
        gather_matrix,
        incoming.reshape(slot_count, atom_w * row_width),
        preferred_element_type=jnp.bfloat16,
    )
    ordered = ordered.reshape(per_dev, atom_w, row_width)
    bounds = lax.dynamic_slice_in_dim(offsets, own_row * per_dev, per_dev + 1)
    lengths = bounds[1:] - bounds[:-1]
    significant = lax.dynamic_slice(mask, (own_row * per_dev, own_col), (per_dev, 1))[:, 0] > 0
    keep_rows = (jnp.arange(atom_w, dtype=jnp.int32)[None, :] < lengths[:, None]) & significant[
        :, None
    ]
    blocks = ordered * keep_rows[:, :, None].astype(jnp.bfloat16)
    kept_rows = blocks.reshape(per_dev * atom_w, row_width)
    coeff_piece = lax.all_gather(coeffs, "col", axis=1, tiled=True)

    def product():
        return lax.dot_general(
            coeff_piece, kept_rows, (((0,), (0,)), ((), ())), preferred_element_type=jnp.float32
        )

    bucket_term = product()
    partial_sums = bucket_term.astype(jnp.bfloat16)
    result = lax.psum_scatter(partial_sums, "row", scatter_dimension=0, tiled=True).astype(
        jnp.float32
    )
    return result.astype(jnp.bfloat16)


def solution(mesh):
    in_specs = (P("row", None, "col"), P("row", "col"), P(), P(), P())
    out_specs = P("row", "col")
    n_row, n_col = mesh.shape["row"], mesh.shape["col"]

    def step(integrals, coeffs, mask, offsets, atom_of_slot):
        even = integrals.shape[0] % (n_row * n_row) == 0
        chosen = line_body if even and n_col == 4 and n_row == 2 * n_col else body
        mapped = jax.shard_map(
            chosen, mesh=mesh, in_specs=in_specs, out_specs=out_specs, check_vma=False
        )
        return mapped(integrals, coeffs, mask, offsets, atom_of_slot)

    return step
```

```python
import functools
import jax
import jax.numpy as jnp
from jax import lax
from jax.experimental import pallas as pl
from jax.experimental.pallas import tpu as pltpu
from jax.sharding import PartitionSpec as P


LANES = 256


def selector(first, alive, atom_w, group):
    pair_w = 3 * atom_w // 2
    rows, cols = group // 2 * pair_w, group * atom_w
    row = lax.broadcasted_iota(jnp.int32, (rows, cols), 0)
    col = lax.broadcasted_iota(jnp.int32, (rows, cols), 1)
    wanted = jnp.full((rows, cols), -1, jnp.int32)
    for pair in range(group // 2):
        inside = row - pair * pair_w
        in_first = inside < first[pair]
        source = jnp.where(in_first, inside, inside + atom_w - first[pair]) + 2 * pair * atom_w
        if alive is not None:
            live = jnp.where(in_first, alive[2 * pair], alive[2 * pair + 1]) > 0
            source = jnp.where(live, source, -1)
        wanted = jnp.where((inside >= 0) & (inside < pair_w), source, wanted)
    return (wanted == col).astype(jnp.bfloat16)


def pack_coeffs_kernel(atom_w, group, per_dev, widths, place, offsets, mine, paired, *pieces):
    step = pl.program_id(0)
    for side, block in enumerate((mine, paired)):
        base = (place[0] if side == 0 else place[0] ^ 1) * per_dev + step * group
        marks = [offsets[base + atom] for atom in range(group)]
        first = [marks[2 * pair + 1] - marks[2 * pair] for pair in range(group // 2)]
        chooser = selector(first, None, atom_w, group)
        begin = 0
        for piece, width in zip(pieces, widths):
            piece[:, side * width : (side + 1) * width] = jnp.dot(
                chooser, block[:, begin : begin + width], preferred_element_type=jnp.float32
            ).astype(jnp.bfloat16)
            begin += width


def pack_coeffs(coeffs, paired, offsets, own_row, per_dev, atom_w, group, widths):
    rows_in, rows_out = group * atom_w, group // 2 * (3 * atom_w // 2)
    steps, half = per_dev // group, paired.shape[1]
    return pl.pallas_call(
        functools.partial(pack_coeffs_kernel, atom_w, group, per_dev, widths),
        grid_spec=pltpu.PrefetchScalarGridSpec(
            num_scalar_prefetch=2,
            grid=(steps,),
            in_specs=[
                pl.BlockSpec((rows_in, half), lambda i, place, offsets: (i, place[0] % 2)),
                pl.BlockSpec((rows_in, half), lambda i, place, offsets: (i, 0)),
            ],
            out_specs=[
                pl.BlockSpec((rows_out, 2 * w), lambda i, place, offsets: (i, 0)) for w in widths
            ],
        ),
        out_shape=[
            jax.ShapeDtypeStruct((steps * rows_out, 2 * w), jnp.bfloat16) for w in widths
        ],
        name="pack_coeffs",
    )(own_row.astype(jnp.int32).reshape(1), offsets, coeffs, paired)


def sort_blocks_kernel(slots, table, blocks, *outs):
    for which, out in enumerate(outs):
        for rank in range(2 * slots):
            out[rank] = blocks[table[which * 2 * slots + rank]]


def sort_blocks(blocks, table, n_chip, slots):
    shape = (2 * slots,) + blocks.shape[1:]
    vmem = pl.BlockSpec(memory_space=pltpu.VMEM)
    return pl.pallas_call(
        functools.partial(sort_blocks_kernel, slots),
        in_specs=[pl.BlockSpec(memory_space=pltpu.SMEM), vmem],
        out_specs=[vmem] * n_chip,
        out_shape=[jax.ShapeDtypeStruct(shape, blocks.dtype)] * n_chip,
        name="sort_blocks",
    )(table, blocks)


def pack_kept_kernel(n_in, slots, atom_w, group, where_of, lengths, alive, *refs):
    arrived, out, stack, window = refs[:n_in], refs[n_in], refs[n_in + 1], refs[n_in + 2]
    for which in range(n_in - 1):
        stack[which * slots : (which + 1) * slots] = arrived[which][:slots]
    stack[(n_in - 1) * slots :] = arrived[n_in - 1][...]
    rows_out = group // 2 * (3 * atom_w // 2)
    for step in range(out.shape[0] // rows_out):
        base = step * group
        for atom in range(group):
            window[atom * atom_w : (atom + 1) * atom_w, :] = stack[where_of[base + atom]]
        first = [lengths[base + 2 * pair] for pair in range(group // 2)]
        chooser = selector(first, [alive[base + i] for i in range(group)], atom_w, group)
        out[step * rows_out : (step + 1) * rows_out, :] = jnp.dot(
            chooser, window[...], preferred_element_type=jnp.float32
        ).astype(jnp.bfloat16)


def pack_kept(arrived, where_of, lengths, alive, atom_w, group):
    slots, width = arrived[0].shape[0] // 2, arrived[0].shape[2]
    per_dev = where_of.shape[0]
    smem, vmem = pl.BlockSpec(memory_space=pltpu.SMEM), pl.BlockSpec(memory_space=pltpu.VMEM)
    return pl.pallas_call(
        functools.partial(pack_kept_kernel, len(arrived), slots, atom_w, group),
        in_specs=[smem] * 3 + [vmem] * len(arrived),
        out_specs=vmem,
        out_shape=jax.ShapeDtypeStruct((per_dev // 2 * (3 * atom_w // 2), width), jnp.bfloat16),
        scratch_shapes=[
            pltpu.VMEM((per_dev, atom_w, width), jnp.bfloat16),
            pltpu.VMEM((group * atom_w, width), jnp.bfloat16),
        ],
        name="pack_kept",
    )(where_of, lengths, alive, *arrived)


def block_tables(atom_of_slot, own_row, n_row, per_dev, slots):
    counter = jnp.arange(per_dev, dtype=jnp.int32)
    holders = atom_of_slot.reshape(n_row, per_dev)
    owner = holders // per_dev
    earlier = (owner[:, None, :] == owner[:, :, None]) & (counter[None, :] < counter[:, None])[None]
    rank = jnp.sum(earlier.astype(jnp.int32), axis=2)
    mine_owner = lax.dynamic_slice_in_dim(owner, own_row, 1)[0]
    mine_rank = lax.dynamic_slice_in_dim(rank, own_row, 1)[0]
    place = (mine_owner ^ own_row) * slots + mine_rank
    table = jnp.sum(jnp.where(place[None, :] == counter[:, None], counter[None, :], 0), axis=1)
    apart = jnp.arange(n_row, dtype=jnp.int32)[:, None] ^ own_row
    arrival = ((apart % 2) * (n_row // 2) + apart // 2) * slots + rank
    local = holders.reshape(-1) - own_row * per_dev
    where_of = jnp.sum(
        jnp.where(local[None, :] == counter[:, None], arrival.reshape(-1)[None, :], 0), axis=1
    )
    return table, where_of


def products_kernel(candidates, choice, kept, kept_pair, *refs):
    n_ref = 1 + max(ref for ref, _, _ in candidates)
    streams, outs = refs[:n_ref], refs[n_ref:-3]
    buffer, held, sems = refs[-3:]
    width = outs[0].shape[0]
    half = width * len(outs)

    def pull(side, ref, offset, place):
        return pltpu.make_async_copy(
            streams[ref].at[:, pl.ds(offset, width)],
            buffer.at[:, pl.ds(side * half + place, width)],
            sems.at[side],
        )

    loads = [
        pltpu.make_async_copy(source, held.at[side], sems.at[2 + side])
        for side, source in enumerate((kept, kept_pair))
    ]
    for side in range(2):
        for step in range(len(outs)):
            for which, (ref, *begin) in enumerate(candidates):

                @pl.when(choice[step] == which)
                def _():
                    pull(side, ref, begin[side], step * width).start()

        loads[side].start()
    total = None
    for side in range(2):
        for step in range(len(outs)):
            pull(side, 0, 0, step * width).wait()
        loads[side].wait()
        term = lax.dot_general(
            buffer[:, side * half : (side + 1) * half],
            held[side],
            (((0,), (0,)), ((), ())),
            preferred_element_type=jnp.float32,
        )
        total = term if total is None else total + term
    for step, out in enumerate(outs):
        out[...] = total[step * width : (step + 1) * width].astype(out.dtype)


def products(choice, kept, kept_pair, streams, candidates, n_out, width):
    rows, columns = kept.shape
    vmem = pl.BlockSpec(memory_space=pltpu.VMEM)
    flops = n_out * 4 * width * rows * columns
    return pl.pallas_call(
        functools.partial(products_kernel, candidates),
        in_specs=[pl.BlockSpec(memory_space=pltpu.SMEM)]
        + [pl.BlockSpec(memory_space=pl.ANY)] * (2 + len(streams)),
        out_specs=[vmem] * n_out,
        out_shape=[jax.ShapeDtypeStruct((width, columns), jnp.bfloat16)] * n_out,
        scratch_shapes=[
            pltpu.VMEM((rows, 2 * n_out * width), jnp.bfloat16),
            pltpu.VMEM((2, rows, columns), jnp.bfloat16),
            pltpu.SemaphoreType.DMA((4,)),
        ],
        cost_estimate=pl.CostEstimate(flops=flops, bytes_accessed=flops // 512, transcendentals=0),
        name="products",
    )(choice, kept, kept_pair, *streams)


def line_body(integrals, coeffs, mask, offsets, atom_of_slot):
    n_row, n_col = lax.axis_size("row"), lax.axis_size("col")
    own_row, own_col = lax.axis_index("row"), lax.axis_index("col")
    per_dev, atom_w, _ = integrals.shape
    slots = per_dev // n_row
    group = LANES // atom_w
    core, chip = own_row % 2, own_row // 2
    n_chip = n_row // 2
    half = coeffs.shape[1] // 2
    widths = (half // 2, half // 4, half // 4)
    n_piece = len(widths)
    last = n_col - 1

    swap = [(r, r ^ 1) for r in range(n_row)]
    other = lax.dynamic_slice_in_dim(coeffs, (1 - core) * half, half, axis=1)
    paired = lax.ppermute(other, "row", swap)
    units = pack_coeffs(coeffs, paired, offsets, own_row, per_dev, atom_w, group, widths)

    right = [(c, c + 1) for c in range(n_col - 1)]
    left = [(c + 1, c) for c in range(n_col - 1)]
    from_left = [lax.ppermute(unit, "col", right) for unit in units]
    from_right = [lax.ppermute(unit, "col", left) for unit in units]

    table, where_of = block_tables(atom_of_slot, own_row, n_row, per_dev, slots)
    bounds = lax.dynamic_slice_in_dim(offsets, own_row * per_dev, per_dev + 1)
    lengths = bounds[1:] - bounds[:-1]
    alive = lax.dynamic_slice(mask, (own_row * per_dev, own_col), (per_dev, 1))[:, 0]
    outgoing = sort_blocks(integrals, table, n_chip, slots)
    arrived = [outgoing[0]] + [
        lax.ppermute(outgoing[d], "row", [(r, r ^ (2 * d)) for r in range(n_row)])
        for d in range(1, n_chip)
    ]
    theirs = jnp.concatenate([block[slots:] for block in arrived], axis=0)
    arrived.append(lax.ppermute(theirs, "row", swap))
    kept = pack_kept(arrived, where_of, lengths, alive, atom_w, group)
    kept_pair = lax.ppermute(kept, "row", swap)

    far_left = [lax.ppermute(unit, "col", right[1:]) for unit in from_left]
    far_right = [lax.ppermute(unit, "col", left[:-1]) for unit in from_right]
    on_left = own_col < n_col // 2
    helped = lax.ppermute(kept, "col", [(0, 1), (last, last - 1)])
    helped_pair = lax.ppermute(helped, "row", swap)

    goals = chip ^ jnp.arange(n_chip, dtype=jnp.int32)
    gap = goals - own_col
    choice = jnp.zeros((n_chip,), jnp.int32)
    for value, which in ((-1, 1), (1, 2), (-2, 3), (2, 4)):
        choice = jnp.where(gap == value, which, choice)
    totals = []
    for which, width in enumerate(widths):
        streams = [
            group_of[which] for group_of in (units, from_left, from_right, far_left, far_right)
        ]
        candidates = tuple((ref, 0, width) for ref in range(len(streams)))
        parts = products(choice, kept, kept_pair, streams, candidates, n_chip, width)
        total = parts[0].astype(jnp.float32)
        for d in range(1, n_chip):
            perm = [(r, r ^ (2 * d)) for r in range(n_row)]
            total = total + lax.ppermute(parts[d], "row", perm).astype(jnp.float32)
        totals.append(lax.optimization_barrier(total.astype(jnp.bfloat16)))

    quarter = half // n_chip
    candidates = []
    for q in range(n_chip):
        begin, piece = q * quarter, 0
        while begin >= widths[piece]:
            begin, piece = begin - widths[piece], piece + 1
        for side in range(2):
            candidates.append((side * n_piece + piece, begin, widths[piece] + begin))
    choice = 2 * goals + on_left.astype(jnp.int32)
    parts = products(
        choice, helped, helped_pair, far_left + far_right, tuple(candidates), n_chip, quarter
    )
    total = parts[0].astype(jnp.float32)
    for d in range(1, n_chip):
        perm = [(r, r ^ (2 * d)) for r in range(n_row)]
        total = total + lax.ppermute(parts[d], "row", perm).astype(jnp.float32)
    total = total.astype(jnp.bfloat16)
    given = []
    for d in range(n_chip):
        perm = [
            (((p ^ d) * 2 + s) * n_col + source, (p * 2 + s) * n_col + goal)
            for source, goal, p in ((1, 0, last), (last - 1, last, 0))
            for s in range(2)
        ]
        given.append(lax.ppermute(total, ("row", "col"), perm))
    is_helped = ((own_col == 0) & (chip == last)) | ((own_col == last) & (chip == 0))
    rows, begin = [], 0
    for total, width in zip(totals, widths):
        gifts = [
            jnp.where(on_left, given[q ^ last], given[q])
            for q in range(begin // quarter, (begin + width) // quarter)
        ]
        rows.append(jnp.where(is_helped, jnp.concatenate(gifts), total))
        begin += width
    return jnp.concatenate(rows, axis=0)


def body(integrals, coeffs, mask, offsets, atom_of_slot):
    n_row = lax.axis_size("row")
    own_row = lax.axis_index("row")
    own_col = lax.axis_index("col")
    per_dev, atom_w, row_width = integrals.shape
    slots_cap = max(2, -(-per_dev // n_row))
    counter = jnp.arange(per_dev, dtype=jnp.int32)
    slot_count = n_row * slots_cap
    mine_slots = lax.dynamic_slice_in_dim(atom_of_slot, own_row * per_dev, per_dev)
    target = mine_slots // per_dev
    before = (target[None, :] == target[:, None]) & (counter[None, :] < counter[:, None])
    arrival_rank = jnp.sum(before.astype(jnp.int32), axis=1)
    position = target * slots_cap + arrival_rank
    placing = (jnp.arange(slot_count, dtype=jnp.int32)[:, None] == position[None, :]).astype(
        jnp.bfloat16
    )
    outgoing = jnp.dot(
        placing, integrals.reshape(per_dev, atom_w * row_width), preferred_element_type=jnp.bfloat16
    )
    outgoing = outgoing.reshape(n_row, slots_cap, atom_w * row_width)
    incoming = lax.all_to_all(outgoing, "row", split_axis=0, concat_axis=0, tiled=True)
    holders = atom_of_slot.reshape(n_row, per_dev)
    is_mine = holders // per_dev == own_row
    arrival = jnp.cumsum(is_mine.astype(jnp.int32), axis=1) - 1
    slot_of = jnp.arange(n_row, dtype=jnp.int32)[:, None] * slots_cap + arrival
    local_atom = holders - own_row * per_dev
    pick_atom = (
        (local_atom.reshape(-1)[:, None] == counter[None, :]) & is_mine.reshape(-1)[:, None]
    ).astype(jnp.float32)
    pick_slot = (
        slot_of.reshape(-1)[:, None] == jnp.arange(slot_count, dtype=jnp.int32)[None, :]
    ).astype(jnp.float32)
    gather_matrix = jnp.dot(pick_atom.T, pick_slot).astype(jnp.bfloat16)
    ordered = jnp.dot(
        gather_matrix,
        incoming.reshape(slot_count, atom_w * row_width),
        preferred_element_type=jnp.bfloat16,
    )
    ordered = ordered.reshape(per_dev, atom_w, row_width)
    bounds = lax.dynamic_slice_in_dim(offsets, own_row * per_dev, per_dev + 1)
    lengths = bounds[1:] - bounds[:-1]
    significant = lax.dynamic_slice(mask, (own_row * per_dev, own_col), (per_dev, 1))[:, 0] > 0
    keep_rows = (jnp.arange(atom_w, dtype=jnp.int32)[None, :] < lengths[:, None]) & significant[
        :, None
    ]
    blocks = ordered * keep_rows[:, :, None].astype(jnp.bfloat16)
    kept_rows = blocks.reshape(per_dev * atom_w, row_width)
    coeff_piece = lax.all_gather(coeffs, "col", axis=1, tiled=True)

    def product():
        return lax.dot_general(
            coeff_piece, kept_rows, (((0,), (0,)), ((), ())), preferred_element_type=jnp.float32
        )

    bucket_term = product()
    partial_sums = bucket_term.astype(jnp.bfloat16)
    result = lax.psum_scatter(partial_sums, "row", scatter_dimension=0, tiled=True).astype(
        jnp.float32
    )
    return result.astype(jnp.bfloat16)


def solution(mesh):
    in_specs = (P("row", None, "col"), P("row", "col"), P(), P(), P())
    out_specs = P("row", "col")
    n_row, n_col = mesh.shape["row"], mesh.shape["col"]

    def step(integrals, coeffs, mask, offsets, atom_of_slot):
        even = integrals.shape[0] % (n_row * n_row) == 0
        chosen = line_body if even and n_col == 4 and n_row == 2 * n_col else body
        mapped = jax.shard_map(
            chosen, mesh=mesh, in_specs=in_specs, out_specs=out_specs, check_vma=False
        )
        return mapped(integrals, coeffs, mask, offsets, atom_of_slot)

    return step
```

```python
import functools
import jax
import jax.numpy as jnp
from jax import lax
from jax.experimental import pallas as pl
from jax.experimental.pallas import tpu as pltpu
from jax.sharding import PartitionSpec as P


LANES = 256


def selector(first, alive, atom_w, group):
    pair_w, cols = 3 * atom_w // 2, group * atom_w
    row = lax.broadcasted_iota(jnp.int32, (pair_w, cols), 0)
    col = lax.broadcasted_iota(jnp.int32, (pair_w, cols), 1)
    bands = []
    for pair in range(group // 2):
        in_first = row < first[pair]
        source = row + jnp.where(in_first, 0, atom_w - first[pair])
        hit = source == col - 2 * pair * atom_w
        if alive is not None:
            live = jnp.where(in_first, alive[2 * pair], alive[2 * pair + 1])
            hit = hit & (live > 0)
        bands.append(jnp.where(hit, 1.0, 0.0).astype(jnp.bfloat16))
    return jnp.concatenate(bands, axis=0)


def pack_coeffs_kernel(atom_w, group, per_dev, widths, here, offsets, coeffs, paired, *refs):
    pieces, held, sems = refs[:-2], refs[-2], refs[-1]
    rows_in, rows_out = group * atom_w, group // 2 * (3 * atom_w // 2)
    half = held.shape[2]
    column = pl.multiple_of(here[0] % 2 * half, half)
    loads = []
    for step in range(per_dev // group):
        rows = pl.ds(step * rows_in, rows_in)
        for side, source in enumerate((coeffs.at[rows, pl.ds(column, half)], paired.at[rows])):
            load = pltpu.make_async_copy(source, held.at[side, rows], sems.at[2 * step + side])
            load.start()
            loads.append(load)
    for step in range(per_dev // group):
        for side in range(2):
            base = (here[0] ^ side) * per_dev + step * group
            marks = [offsets[base + atom] for atom in range(group)]
            first = [marks[2 * pair + 1] - marks[2 * pair] for pair in range(group // 2)]
            chooser = selector(first, None, atom_w, group)
            loads[2 * step + side].wait()
            block = held[side, step * rows_in : (step + 1) * rows_in]
            packed = jnp.dot(chooser, block, preferred_element_type=jnp.float32)
            packed = packed.astype(jnp.bfloat16)
            begin = 0
            for piece, width in zip(pieces, widths):
                piece[
                    step * rows_out : (step + 1) * rows_out, side * width : (side + 1) * width
                ] = packed[:, begin : begin + width]
                begin += width


def pack_coeffs(coeffs, paired, offsets, own_row, per_dev, atom_w, group, widths):
    steps, rows_out = per_dev // group, group // 2 * (3 * atom_w // 2)
    smem, vmem = pl.BlockSpec(memory_space=pltpu.SMEM), pl.BlockSpec(memory_space=pltpu.VMEM)
    return pl.pallas_call(
        functools.partial(pack_coeffs_kernel, atom_w, group, per_dev, widths),
        in_specs=[smem, smem] + [pl.BlockSpec(memory_space=pl.ANY)] * 2,
        out_specs=[vmem] * len(widths),
        out_shape=[
            jax.ShapeDtypeStruct((steps * rows_out, 2 * w), jnp.bfloat16) for w in widths
        ],
        scratch_shapes=[
            pltpu.VMEM((2,) + paired.shape, jnp.bfloat16),
            pltpu.SemaphoreType.DMA((2 * steps,)),
        ],
        name="pack_coeffs",
    )(own_row.astype(jnp.int32).reshape(1), offsets, coeffs, paired)


def sort_blocks_kernel(slots, table, blocks, *outs):
    for which, out in enumerate(outs):
        for rank in range(2 * slots):
            out[rank] = blocks[table[which * 2 * slots + rank]]


def sort_blocks(blocks, table, n_chip, slots):
    shape = (2 * slots,) + blocks.shape[1:]
    vmem = pl.BlockSpec(memory_space=pltpu.VMEM)
    return pl.pallas_call(
        functools.partial(sort_blocks_kernel, slots),
        in_specs=[pl.BlockSpec(memory_space=pltpu.SMEM), vmem],
        out_specs=[vmem] * n_chip,
        out_shape=[jax.ShapeDtypeStruct(shape, blocks.dtype)] * n_chip,
        name="sort_blocks",
    )(table, blocks)


def pack_kept_kernel(n_in, slots, atom_w, group, where_of, lengths, alive, *refs):
    arrived, out, stack, window = refs[:n_in], refs[n_in], refs[n_in + 1], refs[n_in + 2]
    for which in range(n_in - 1):
        stack[which * slots : (which + 1) * slots] = arrived[which][:slots]
    stack[(n_in - 1) * slots :] = arrived[n_in - 1][...]
    rows_out = group // 2 * (3 * atom_w // 2)
    for step in range(out.shape[0] // rows_out):
        base = step * group
        for atom in range(group):
            window[atom * atom_w : (atom + 1) * atom_w, :] = stack[where_of[base + atom]]
        first = [lengths[base + 2 * pair] for pair in range(group // 2)]
        chooser = selector(first, [alive[base + i] for i in range(group)], atom_w, group)
        out[step * rows_out : (step + 1) * rows_out, :] = jnp.dot(
            chooser, window[...], preferred_element_type=jnp.float32
        ).astype(jnp.bfloat16)


def pack_kept(arrived, where_of, lengths, alive, atom_w, group):
    slots, width = arrived[0].shape[0] // 2, arrived[0].shape[2]
    per_dev = where_of.shape[0]
    smem, vmem = pl.BlockSpec(memory_space=pltpu.SMEM), pl.BlockSpec(memory_space=pltpu.VMEM)
    return pl.pallas_call(
        functools.partial(pack_kept_kernel, len(arrived), slots, atom_w, group),
        in_specs=[smem] * 3 + [vmem] * len(arrived),
        out_specs=vmem,
        out_shape=jax.ShapeDtypeStruct((per_dev // 2 * (3 * atom_w // 2), width), jnp.bfloat16),
        scratch_shapes=[
            pltpu.VMEM((per_dev, atom_w, width), jnp.bfloat16),
            pltpu.VMEM((group * atom_w, width), jnp.bfloat16),
        ],
        name="pack_kept",
    )(where_of, lengths, alive, *arrived)


def block_tables(atom_of_slot, own_row, n_row, per_dev, slots):
    counter = jnp.arange(per_dev, dtype=jnp.int32)
    holders = atom_of_slot.reshape(n_row, per_dev)
    owner = holders // per_dev
    earlier = (owner[:, None, :] == owner[:, :, None]) & (counter[None, :] < counter[:, None])[None]
    rank = jnp.sum(earlier.astype(jnp.int32), axis=2)
    mine_owner = lax.dynamic_slice_in_dim(owner, own_row, 1)[0]
    mine_rank = lax.dynamic_slice_in_dim(rank, own_row, 1)[0]
    place = (mine_owner ^ own_row) * slots + mine_rank
    table = jnp.sum(jnp.where(place[None, :] == counter[:, None], counter[None, :], 0), axis=1)
    apart = jnp.arange(n_row, dtype=jnp.int32)[:, None] ^ own_row
    arrival = ((apart % 2) * (n_row // 2) + apart // 2) * slots + rank
    local = holders.reshape(-1) - own_row * per_dev
    where_of = jnp.sum(
        jnp.where(local[None, :] == counter[:, None], arrival.reshape(-1)[None, :], 0), axis=1
    )
    return table, where_of


def products_kernel(candidates, choice, kept, kept_pair, *refs):
    n_ref = 1 + max(ref for ref, _, _ in candidates)
    streams, outs = refs[:n_ref], refs[n_ref:-3]
    buffer, held, sems = refs[-3:]
    width = outs[0].shape[0]
    half = width * len(outs)

    def pull(side, ref, offset, place):
        return pltpu.make_async_copy(
            streams[ref].at[:, pl.ds(offset, width)],
            buffer.at[:, pl.ds(side * half + place, width)],
            sems.at[side],
        )

    loads = [
        pltpu.make_async_copy(source, held.at[side], sems.at[2 + side])
        for side, source in enumerate((kept, kept_pair))
    ]
    for side in range(2):
        for step in range(len(outs)):
            for which, (ref, *begin) in enumerate(candidates):

                @pl.when(choice[step] == which)
                def _():
                    pull(side, ref, begin[side], step * width).start()

        loads[side].start()
    total = None
    for side in range(2):
        for step in range(len(outs)):
            pull(side, 0, 0, step * width).wait()
        loads[side].wait()
        term = lax.dot_general(
            buffer[:, side * half : (side + 1) * half],
            held[side],
            (((0,), (0,)), ((), ())),
            preferred_element_type=jnp.float32,
        )
        total = term if total is None else total + term
    for step, out in enumerate(outs):
        out[...] = total[step * width : (step + 1) * width].astype(out.dtype)


def products(choice, kept, kept_pair, streams, candidates, n_out, width):
    rows, columns = kept.shape
    vmem = pl.BlockSpec(memory_space=pltpu.VMEM)
    flops = n_out * 4 * width * rows * columns
    return pl.pallas_call(
        functools.partial(products_kernel, candidates),
        in_specs=[pl.BlockSpec(memory_space=pltpu.SMEM)]
        + [pl.BlockSpec(memory_space=pl.ANY)] * (2 + len(streams)),
        out_specs=[vmem] * n_out,
        out_shape=[jax.ShapeDtypeStruct((width, columns), jnp.bfloat16)] * n_out,
        scratch_shapes=[
            pltpu.VMEM((rows, 2 * n_out * width), jnp.bfloat16),
            pltpu.VMEM((2, rows, columns), jnp.bfloat16),
            pltpu.SemaphoreType.DMA((4,)),
        ],
        cost_estimate=pl.CostEstimate(flops=flops, bytes_accessed=flops // 512, transcendentals=0),
        name="products",
    )(choice, kept, kept_pair, *streams)


def line_body(integrals, coeffs, mask, offsets, atom_of_slot):
    n_row, n_col = lax.axis_size("row"), lax.axis_size("col")
    own_row, own_col = lax.axis_index("row"), lax.axis_index("col")
    per_dev, atom_w, _ = integrals.shape
    slots = per_dev // n_row
    group = LANES // atom_w
    core, chip = own_row % 2, own_row // 2
    n_chip = n_row // 2
    half = coeffs.shape[1] // 2
    widths = (half // 2, half // 4, half // 4)
    n_piece = len(widths)
    last = n_col - 1

    swap = [(r, r ^ 1) for r in range(n_row)]
    other = lax.dynamic_slice_in_dim(coeffs, (1 - core) * half, half, axis=1)
    paired = lax.ppermute(other, "row", swap)
    units = pack_coeffs(coeffs, paired, offsets, own_row, per_dev, atom_w, group, widths)

    right = [(c, c + 1) for c in range(n_col - 1)]
    left = [(c + 1, c) for c in range(n_col - 1)]
    from_left = [lax.ppermute(unit, "col", right) for unit in units]
    from_right = [lax.ppermute(unit, "col", left) for unit in units]

    table, where_of = block_tables(atom_of_slot, own_row, n_row, per_dev, slots)
    bounds = lax.dynamic_slice_in_dim(offsets, own_row * per_dev, per_dev + 1)
    lengths = bounds[1:] - bounds[:-1]
    alive = lax.dynamic_slice(mask, (own_row * per_dev, own_col), (per_dev, 1))[:, 0]
    outgoing = sort_blocks(integrals, table, n_chip, slots)
    arrived = [outgoing[0]] + [
        lax.ppermute(outgoing[d], "row", [(r, r ^ (2 * d)) for r in range(n_row)])
        for d in range(1, n_chip)
    ]
    theirs = jnp.concatenate([block[slots:] for block in arrived], axis=0)
    arrived.append(lax.ppermute(theirs, "row", swap))
    kept = pack_kept(arrived, where_of, lengths, alive, atom_w, group)
    kept_pair = lax.ppermute(kept, "row", swap)

    far_left = [lax.ppermute(unit, "col", right[1:]) for unit in from_left]
    far_right = [lax.ppermute(unit, "col", left[:-1]) for unit in from_right]
    on_left = own_col < n_col // 2
    helped = lax.ppermute(kept, "col", [(0, 1), (last, last - 1)])
    helped_pair = lax.ppermute(helped, "row", swap)

    goals = chip ^ jnp.arange(n_chip, dtype=jnp.int32)
    gap = goals - own_col
    choice = jnp.zeros((n_chip,), jnp.int32)
    for value, which in ((-1, 1), (1, 2), (-2, 3), (2, 4)):
        choice = jnp.where(gap == value, which, choice)
    totals = []
    for which, width in enumerate(widths):
        streams = [
            group_of[which] for group_of in (units, from_left, from_right, far_left, far_right)
        ]
        candidates = tuple((ref, 0, width) for ref in range(len(streams)))
        parts = products(choice, kept, kept_pair, streams, candidates, n_chip, width)
        total = parts[0].astype(jnp.float32)
        for d in range(1, n_chip):
            perm = [(r, r ^ (2 * d)) for r in range(n_row)]
            total = total + lax.ppermute(parts[d], "row", perm).astype(jnp.float32)
        totals.append(lax.optimization_barrier(total.astype(jnp.bfloat16)))

    quarter = half // n_chip
    candidates = []
    for q in range(n_chip):
        begin, piece = q * quarter, 0
        while begin >= widths[piece]:
            begin, piece = begin - widths[piece], piece + 1
        for side in range(2):
            candidates.append((side * n_piece + piece, begin, widths[piece] + begin))
    choice = 2 * goals + on_left.astype(jnp.int32)
    parts = products(
        choice, helped, helped_pair, far_left + far_right, tuple(candidates), n_chip, quarter
    )
    total = parts[0].astype(jnp.float32)
    for d in range(1, n_chip):
        perm = [(r, r ^ (2 * d)) for r in range(n_row)]
        total = total + lax.ppermute(parts[d], "row", perm).astype(jnp.float32)
    total = total.astype(jnp.bfloat16)
    given = []
    for d in range(n_chip):
        perm = [
            (((p ^ d) * 2 + s) * n_col + source, (p * 2 + s) * n_col + goal)
            for source, goal, p in ((1, 0, last), (last - 1, last, 0))
            for s in range(2)
        ]
        given.append(lax.ppermute(total, ("row", "col"), perm))
    is_helped = ((own_col == 0) & (chip == last)) | ((own_col == last) & (chip == 0))
    rows, begin = [], 0
    for total, width in zip(totals, widths):
        gifts = [
            jnp.where(on_left, given[q ^ last], given[q])
            for q in range(begin // quarter, (begin + width) // quarter)
        ]
        rows.append(jnp.where(is_helped, jnp.concatenate(gifts), total))
        begin += width
    return jnp.concatenate(rows, axis=0)


def body(integrals, coeffs, mask, offsets, atom_of_slot):
    n_row = lax.axis_size("row")
    own_row = lax.axis_index("row")
    own_col = lax.axis_index("col")
    per_dev, atom_w, row_width = integrals.shape
    slots_cap = max(2, -(-per_dev // n_row))
    counter = jnp.arange(per_dev, dtype=jnp.int32)
    slot_count = n_row * slots_cap
    mine_slots = lax.dynamic_slice_in_dim(atom_of_slot, own_row * per_dev, per_dev)
    target = mine_slots // per_dev
    before = (target[None, :] == target[:, None]) & (counter[None, :] < counter[:, None])
    arrival_rank = jnp.sum(before.astype(jnp.int32), axis=1)
    position = target * slots_cap + arrival_rank
    placing = (jnp.arange(slot_count, dtype=jnp.int32)[:, None] == position[None, :]).astype(
        jnp.bfloat16
    )
    outgoing = jnp.dot(
        placing, integrals.reshape(per_dev, atom_w * row_width), preferred_element_type=jnp.bfloat16
    )
    outgoing = outgoing.reshape(n_row, slots_cap, atom_w * row_width)
    incoming = lax.all_to_all(outgoing, "row", split_axis=0, concat_axis=0, tiled=True)
    holders = atom_of_slot.reshape(n_row, per_dev)
    is_mine = holders // per_dev == own_row
    arrival = jnp.cumsum(is_mine.astype(jnp.int32), axis=1) - 1
    slot_of = jnp.arange(n_row, dtype=jnp.int32)[:, None] * slots_cap + arrival
    local_atom = holders - own_row * per_dev
    pick_atom = (
        (local_atom.reshape(-1)[:, None] == counter[None, :]) & is_mine.reshape(-1)[:, None]
    ).astype(jnp.float32)
    pick_slot = (
        slot_of.reshape(-1)[:, None] == jnp.arange(slot_count, dtype=jnp.int32)[None, :]
    ).astype(jnp.float32)
    gather_matrix = jnp.dot(pick_atom.T, pick_slot).astype(jnp.bfloat16)
    ordered = jnp.dot(
        gather_matrix,
        incoming.reshape(slot_count, atom_w * row_width),
        preferred_element_type=jnp.bfloat16,
    )
    ordered = ordered.reshape(per_dev, atom_w, row_width)
    bounds = lax.dynamic_slice_in_dim(offsets, own_row * per_dev, per_dev + 1)
    lengths = bounds[1:] - bounds[:-1]
    significant = lax.dynamic_slice(mask, (own_row * per_dev, own_col), (per_dev, 1))[:, 0] > 0
    keep_rows = (jnp.arange(atom_w, dtype=jnp.int32)[None, :] < lengths[:, None]) & significant[
        :, None
    ]
    blocks = ordered * keep_rows[:, :, None].astype(jnp.bfloat16)
    kept_rows = blocks.reshape(per_dev * atom_w, row_width)
    coeff_piece = lax.all_gather(coeffs, "col", axis=1, tiled=True)

    def product():
        return lax.dot_general(
            coeff_piece, kept_rows, (((0,), (0,)), ((), ())), preferred_element_type=jnp.float32
        )

    bucket_term = product()
    partial_sums = bucket_term.astype(jnp.bfloat16)
    result = lax.psum_scatter(partial_sums, "row", scatter_dimension=0, tiled=True).astype(
        jnp.float32
    )
    return result.astype(jnp.bfloat16)


def solution(mesh):
    in_specs = (P("row", None, "col"), P("row", "col"), P(), P(), P())
    out_specs = P("row", "col")
    n_row, n_col = mesh.shape["row"], mesh.shape["col"]

    def step(integrals, coeffs, mask, offsets, atom_of_slot):
        even = integrals.shape[0] % (n_row * n_row) == 0
        chosen = line_body if even and n_col == 4 and n_row == 2 * n_col else body
        mapped = jax.shard_map(
            chosen, mesh=mesh, in_specs=in_specs, out_specs=out_specs, check_vma=False
        )
        return mapped(integrals, coeffs, mask, offsets, atom_of_slot)

    return step
```
